64 devices in a mesh: batch: 4 (over x, y), rows: 16 (over z, core).
Axes of the slice: x: 2, y: 2, z: 8, core: 2. Of those that a mesh axis runs over, the one named last changes fastest.
The devices are a block of a 4x4x8 slice.
Arguments:
- a_mat: float32 [524288, 640], P(('batch', 'rows')), parts along dimension 0
- rhs: float32 [524288, 64], P(('batch', 'rows')), parts along dimension 0
Outputs:
- output 1: float32 [2560, 64], P('batch'), parts along dimension 0
- output 2: float32 [2560, 640], P('batch'), parts along dimension 0
There are 4 independent parts. The reference program is written for one: setup_inputs(seed, part) draws one part's arguments, and reference() takes and returns one part's arrays. A program takes and returns all parts, laid end to end along the dimension named above; each array names one.
All inputs are finite; a program needn't handle non-finite values.
Results may differ from the reference program's by a relative error of at most 0.001.
Values sent between devices are 32-bit elements.
A program may use at most 768 MiB of HBM per device.

```python
import jax
import jax.numpy as jnp
from jax import lax
import math

M_ROWS = 131072
N_COLS = 640
N_RHS = 64
SHARDS = 16
COND_NUMBER = 1000.0
NOISE_LEVEL = 0.001


def setup_inputs(seed: int = 0, part: int = 0) -> dict:
    part_key = jax.random.fold_in(jax.random.key(seed), part)
    key_base, key_mix, key_sol, key_noise = jax.random.split(part_key, 4)
    rows_per = M_ROWS // SHARDS
    base = jax.random.normal(key_base, (M_ROWS, N_COLS), jnp.float32)
    row_shard = jnp.arange(M_ROWS) // rows_per
    col_owner = jnp.arange(N_COLS) % SHARDS
    low_weight = 0.5 / math.sqrt(SHARDS)
    weights = jnp.where(row_shard[:, None] == col_owner[None, :], 1.0, low_weight)
    col_scale = 1.0 / math.sqrt(rows_per * (1.0 + 0.25 * (SHARDS - 1) / SHARDS))
    basis = base * weights * col_scale
    ortho = jnp.linalg.qr(jax.random.normal(key_mix, (N_COLS, N_COLS), jnp.float32))[0]
    tail_len = N_COLS // 4
    tail_pos = jnp.clip((jnp.arange(N_COLS) - (N_COLS - tail_len)) / (tail_len - 1), 0.0, 1.0)
    sigma = jnp.power(COND_NUMBER, -tail_pos)
    upper_c = jnp.linalg.qr(sigma[:, None] * ortho.T)[1] * math.sqrt(N_COLS)
    a_mat = jnp.dot(basis, upper_c, precision=lax.Precision.HIGHEST)
    x_true = jax.random.normal(key_sol, (N_COLS, N_RHS), jnp.float32)
    signal = jnp.dot(a_mat, x_true, precision=lax.Precision.HIGHEST)
    noise_scale = NOISE_LEVEL * jnp.sqrt(jnp.mean(signal * signal))
    rhs = signal + noise_scale * jax.random.normal(key_noise, (M_ROWS, N_RHS), jnp.float32)
    return {"a_mat": a_mat.astype(jnp.float32), "rhs": rhs.astype(jnp.float32)}


def reference(a_mat, rhs):
    highest = lax.Precision.HIGHEST
    gram_one = jnp.dot(a_mat.T, a_mat, precision=highest, preferred_element_type=jnp.float32)
    low_one = jnp.linalg.cholesky(gram_one)
    q_one = lax.linalg.triangular_solve(low_one, a_mat, left_side=False, lower=True, transpose_a=True)
    gram_two = jnp.dot(q_one.T, q_one, precision=highest, preferred_element_type=jnp.float32)
    low_two = jnp.linalg.cholesky(gram_two)
    proj_one = jnp.dot(q_one.T, rhs, precision=highest, preferred_element_type=jnp.float32)
    proj_two = lax.linalg.triangular_solve(low_two, proj_one, left_side=True, lower=True)
    upper_r = jnp.dot(low_two.T, low_one.T, precision=highest, preferred_element_type=jnp.float32)
    x_sol = lax.linalg.triangular_solve(upper_r, proj_two, left_side=True, lower=False)
    return (x_sol, upper_r)
```

```python
import functools
import jax
import jax.numpy as jnp
from jax import lax
from jax.experimental import pallas as pl
from jax.experimental.pallas import tpu as pltpu
from jax.sharding import PartitionSpec as P

HIGHEST = lax.Precision.HIGHEST
MESH = pl.DeviceIdType.MESH
LEAF = 8
BLK = 128
WIDE = 256
ROW_TILE = 512
VMEM_BYTES = 64000 * 1024


def dot_f32(lhs, rhs, lhs_dim, rhs_dim):
    return lax.dot_general(lhs, rhs, (((lhs_dim,), (rhs_dim,)), ((), ())), precision=HIGHEST, preferred_element_type=jnp.float32)


def block_pairs(n):
    n_blk = n // BLK
    return [(i, j) for i in range(n_blk) for j in range(i, n_blk)]


def packed_rows(n, n_rhs, members):
    rows = len(block_pairs(n)) * BLK + (n // 2 if n_rhs else 0)
    unit = 8 * members
    return -(-rows // unit) * unit


def pack_upper(acc, out_ref, n):
    for idx, (i, j) in enumerate(block_pairs(n)):
        out_ref[idx * BLK:(idx + 1) * BLK, :] = acc[i * BLK:(i + 1) * BLK, j * BLK:(j + 1) * BLK]


def gram_kernel(a_ref, out_ref, acc):
    n = a_ref.shape[1]

    @pl.when(pl.program_id(0) == 0)
    def _():
        acc[...] = jnp.zeros_like(acc)

    for lo in range(0, n, WIDE):
        hi = min(lo + WIDE, n)
        acc[:hi, lo:hi] += dot_f32(a_ref[:, :hi], a_ref[:, lo:hi], 0, 0)

    @pl.when(pl.program_id(0) == pl.num_programs(0) - 1)
    def _():
        pack_upper(acc, out_ref, n)


def local_gram(a_blk, rows):
    m, n = a_blk.shape
    return pl.pallas_call(
        gram_kernel,
        grid=(m // ROW_TILE,),
        out_shape=jax.ShapeDtypeStruct((rows, BLK), jnp.float32),
        in_specs=[pl.BlockSpec((ROW_TILE, n), lambda t: (t, 0))],
        out_specs=pl.BlockSpec((rows, BLK), lambda t: (0, 0)),
        scratch_shapes=[pltpu.VMEM((n, n), jnp.float32)],
        compiler_params=pltpu.CompilerParams(vmem_limit_bytes=VMEM_BYTES),
        cost_estimate=pl.CostEstimate(flops=m * n * n * 6, bytes_accessed=4 * m * n, transcendentals=0),
        name="gram_one",
    )(a_blk)


def basis_kernel(a_ref, b_ref, inv_ref, out_ref, acc, proj, q_ref):
    n, n_rhs = a_ref.shape[1], b_ref.shape[1]

    @pl.when(pl.program_id(0) == 0)
    def _():
        acc[...] = jnp.zeros_like(acc)
        proj[...] = jnp.zeros_like(proj)

    for lo in range(0, n, WIDE):
        hi = min(lo + WIDE, n)
        q_ref[:, lo:hi] = dot_f32(a_ref[:, :hi], inv_ref[:hi, lo:hi], 1, 0)
    for lo in range(0, n, WIDE):
        hi = min(lo + WIDE, n)
        if hi < n:
            acc[:hi, lo:hi] += dot_f32(q_ref[:, :hi], q_ref[:, lo:hi], 0, 0)
        else:
            both = dot_f32(q_ref[...], jnp.concatenate([q_ref[:, lo:hi], b_ref[...]], axis=1), 0, 0)
            acc[:, lo:hi] += both[:, :hi - lo]
            proj[...] += both[:, hi - lo:]

    @pl.when(pl.program_id(0) == pl.num_programs(0) - 1)
    def _():
        pack_upper(acc, out_ref, n)
        base = len(block_pairs(n)) * BLK
        half = n // 2
        out_ref[base:base + half, :] = jnp.concatenate([proj[:half, :], proj[half:, :]], axis=1)
        if base + half < out_ref.shape[0]:
            out_ref[base + half:, :] = jnp.zeros((out_ref.shape[0] - base - half, BLK), jnp.float32)


def local_basis(a_blk, b_blk, r_inv, rows):
    m, n = a_blk.shape
    n_rhs = b_blk.shape[1]
    return pl.pallas_call(
        basis_kernel,
        grid=(m // ROW_TILE,),
        out_shape=jax.ShapeDtypeStruct((rows, BLK), jnp.float32),
        in_specs=[
            pl.BlockSpec((ROW_TILE, n), lambda t: (t, 0)),
            pl.BlockSpec((ROW_TILE, n_rhs), lambda t: (t, 0)),
            pl.BlockSpec((n, n), lambda t: (0, 0)),
        ],
        out_specs=pl.BlockSpec((rows, BLK), lambda t: (0, 0)),
        scratch_shapes=[pltpu.VMEM((n, n), jnp.float32), pltpu.VMEM((n, n_rhs), jnp.float32), pltpu.VMEM((ROW_TILE, n), jnp.float32)],
        compiler_params=pltpu.CompilerParams(vmem_limit_bytes=VMEM_BYTES),
        cost_estimate=pl.CostEstimate(flops=m * n * n * 12, bytes_accessed=4 * m * (n + n_rhs), transcendentals=0),
        name="basis_gram_two",
    )(a_blk, b_blk, r_inv)


def sum_kernel(members, part, out, pair_buf, acc, slots, pair_send, pair_recv, send_sems, recv_sems, back_send, back_recv, fwd_send, fwd_recv):
    chips = members // 2
    me = lax.axis_index("rows")
    core, chip = lax.rem(me, 2), lax.div(me, 2)
    half = part.shape[0] // 2
    chunk = half // chips
    pair = {"rows": chip * 2 + 1 - core}

    def peer(d):
        return lax.rem(chip + d, chips)

    def rows_at(start, size):
        return pl.ds(pl.multiple_of(start, 8), size)

    barrier = pltpu.get_barrier_semaphore()
    pl.semaphore_signal(barrier, inc=1, device_id=pair, device_id_type=MESH)
    for d in range(1, chips):
        pl.semaphore_signal(barrier, inc=1, device_id={"rows": peer(d) * 2 + core}, device_id_type=MESH)
    pl.semaphore_wait(barrier, chips)

    swap = pltpu.make_async_remote_copy(
        src_ref=part.at[rows_at((1 - core) * half, half)], dst_ref=pair_buf, send_sem=pair_send, recv_sem=pair_recv,
        device_id=pair, device_id_type=MESH)
    swap.start()
    swap.wait()
    mine = core * half
    acc[...] = part[rows_at(mine, half)] + pair_buf[...]

    out_copies = []
    for d in range(1, chips):
        copy = pltpu.make_async_remote_copy(
            src_ref=acc.at[rows_at(peer(d) * chunk, chunk)], dst_ref=slots.at[d - 1], send_sem=send_sems.at[d - 1], recv_sem=recv_sems.at[d - 1],
            device_id={"rows": peer(d) * 2 + core}, device_id_type=MESH)
        copy.start()
        out_copies.append(copy)
    for copy in out_copies:
        copy.wait()
    total = acc[rows_at(chip * chunk, chunk)]
    for d in range(1, chips):
        total = total + slots[d - 1]
    own = rows_at(mine + chip * chunk, chunk)
    out[own] = total

    back_copies = []
    for d in range(1, chips):
        copy = pltpu.make_async_remote_copy(
            src_ref=out.at[own], dst_ref=out.at[own], send_sem=back_send.at[d - 1], recv_sem=back_recv.at[d - 1],
            device_id={"rows": peer(d) * 2 + core}, device_id_type=MESH)
        copy.start()
        back_copies.append(copy)
    forwards = []
    for d in range(chips):
        if d:
            back_copies[d - 1].wait_recv()
        src = rows_at(mine + peer(chips - d) * chunk, chunk)
        copy = pltpu.make_async_remote_copy(
            src_ref=out.at[src], dst_ref=out.at[src], send_sem=fwd_send.at[d], recv_sem=fwd_recv.at[d],
            device_id=pair, device_id_type=MESH)
        copy.start()
        forwards.append(copy)
    for copy in back_copies:
        copy.wait_send()
    for copy in forwards:
        copy.wait()


def sum_over_rows(part, members, collective_id):
    rows = part.shape[0]
    chips = members // 2
    half = rows // 2
    chunk = half // chips
    sems = pltpu.SemaphoreType.DMA
    return pl.pallas_call(
        functools.partial(sum_kernel, members),
        out_shape=jax.ShapeDtypeStruct(part.shape, jnp.float32),
        in_specs=[pl.BlockSpec(memory_space=pltpu.VMEM)],
        out_specs=pl.BlockSpec(memory_space=pltpu.VMEM),
        scratch_shapes=[
            pltpu.VMEM((half, BLK), jnp.float32), pltpu.VMEM((half, BLK), jnp.float32), pltpu.VMEM((chips - 1, chunk, BLK), jnp.float32),
            sems, sems, sems((chips - 1,)), sems((chips - 1,)), sems((chips - 1,)), sems((chips - 1,)), sems((chips,)), sems((chips,)),
        ],
        compiler_params=pltpu.CompilerParams(collective_id=collective_id, has_side_effects=True),
        name="sum_over_rows",
    )(part)


def row_of(arr, idx):
    return jnp.broadcast_to(arr[idx:idx + 1, :], (LEAF, arr.shape[1]))


def factor_block(sym):
    n_leaf = BLK // LEAF
    ahead = 2
    row_id = lax.broadcasted_iota(jnp.int32, (BLK, BLK), 0)
    col_id = lax.broadcasted_iota(jnp.int32, (BLK, BLK), 1)
    eye = (row_id == col_id).astype(jnp.float32)
    sub_id = lax.broadcasted_iota(jnp.int32, (LEAF, BLK), 0)
    s_rows = [sym[LEAF * t:LEAF * (t + 1), :] for t in range(n_leaf)]
    i_rows = [eye[LEAF * t:LEAF * (t + 1), :] for t in range(n_leaf)]
    for t in range(n_leaf):
        span = list(range(t, min(t + ahead + 1, n_leaf)))
        ecol = [[jnp.broadcast_to(s_rows[u][:, LEAF * t + i:LEAF * t + i + 1], (LEAF, BLK)) for u in span] for i in range(LEAF)]
        w_s, w_i = s_rows[t], i_rows[t]
        for i in range(LEAF):
            inv = lax.rsqrt(row_of(ecol[i][0], i))
            lcol = [e * inv for e in ecol[i]]
            bc_s = row_of(s_rows[t], i) * inv
            bc_i = row_of(i_rows[t], i) * inv
            w_s = jnp.where(sub_id == i, bc_s, w_s)
            w_i = jnp.where(sub_id == i, bc_i, w_i)
            for v, u in enumerate(span):
                if v == 0 and i == LEAF - 1:
                    continue
                s_rows[u] = s_rows[u] - lcol[v] * bc_s
                i_next = i_rows[u] - lcol[v] * bc_i
                i_rows[u] = i_next if v else jnp.where(sub_id > i, i_next, i_rows[u])
            for j in range(i + 1, LEAF):
                piv = row_of(lcol[0], j)
                ecol[j] = [e - c * piv for e, c in zip(ecol[j], lcol)]
        s_rows[t], i_rows[t] = w_s, w_i
        rest = t + ahead + 1
        if rest < n_leaf:
            upd = dot_f32(w_s, jnp.concatenate([w_s, w_i], axis=1), 0, 0)
            for u in range(rest, n_leaf):
                s_rows[u] = s_rows[u] - upd[LEAF * u:LEAF * (u + 1), :BLK]
                i_rows[u] = i_rows[u] - upd[LEAF * u:LEAF * (u + 1), BLK:]
    r_blk = jnp.where(row_id <= col_id, jnp.concatenate(s_rows, axis=0), 0.0)
    linv = jnp.where(row_id >= col_id, jnp.concatenate(i_rows, axis=0), 0.0)
    return r_blk, linv


def factor_all(work, r_out, n):
    n_blk = n // BLK

    def step(k, carry):
        base = pl.multiple_of(k * BLK, BLK)
        r_blk, linv = factor_block(work[pl.ds(base, BLK), pl.ds(base, BLK)])
        for kk in range(n_blk):
            @pl.when(k == kk)
            def _():
                lo, hi = BLK * kk, BLK * (kk + 1)
                if lo:
                    work[lo:hi, :lo] = dot_f32(linv, work[lo:hi, :lo], 1, 0)
                    r_out[lo:hi, :lo] = jnp.zeros((BLK, lo), jnp.float32)
                work[lo:hi, lo:hi] = linv
                r_out[lo:hi, lo:hi] = r_blk
                if hi < n:
                    r_row = dot_f32(linv, work[lo:hi, hi:], 1, 0)
                    r_out[lo:hi, hi:] = r_row
                    work[lo:hi, hi:] = jnp.zeros((BLK, n - hi), jnp.float32)
                    for ii in range(kk + 1, n_blk):
                        a, b = BLK * ii, BLK * (ii + 1)
                        fac = r_row[:, a - hi:b - hi]
                        work[a:b, a:] = work[a:b, a:] - dot_f32(fac, r_row[:, a - hi:], 0, 0)
                        if lo:
                            work[a:b, :lo] = work[a:b, :lo] - dot_f32(fac, work[lo:hi, :lo], 0, 0)
                        work[a:b, lo:hi] = -dot_f32(fac, linv, 0, 0)
        return carry

    lax.fori_loop(0, n_blk, step, 0)


def unpack_upper(packed, work, n):
    for idx, (i, j) in enumerate(block_pairs(n)):
        work[i * BLK:(i + 1) * BLK, j * BLK:(j + 1) * BLK] = packed[idx * BLK:(idx + 1) * BLK, :]
        if i < j:
            work[j * BLK:(j + 1) * BLK, i * BLK:(i + 1) * BLK] = jnp.zeros((BLK, BLK), jnp.float32)


def factor_kernel(packed, r_out, inv_out, work):
    n = work.shape[0]
    unpack_upper(packed, work, n)
    factor_all(work, r_out, n)
    for c in range(0, n, BLK):
        inv_out[:, c:c + BLK] = work[c:c + BLK, :].T


def factor_one(packed, n):
    return pl.pallas_call(
        factor_kernel,
        out_shape=[jax.ShapeDtypeStruct((n, n), jnp.float32)] * 2,
        in_specs=[pl.BlockSpec(memory_space=pltpu.VMEM)],
        out_specs=[pl.BlockSpec(memory_space=pltpu.VMEM)] * 2,
        scratch_shapes=[pltpu.VMEM((n, n), jnp.float32)],
        name="factor_one",
    )(packed)


def finish_kernel(packed, r_one, inv_one, x_out, r_out, work, r_two):
    n, n_rhs = x_out.shape
    unpack_upper(packed, work, n)
    factor_all(work, r_two, n)
    base = len(block_pairs(n)) * BLK
    half = n // 2
    flat = packed[base:base + half, :]
    proj = jnp.concatenate([flat[:, :n_rhs], flat[:, n_rhs:]], axis=0)
    proj_two = dot_f32(work[...], proj, 1, 0)
    back = dot_f32(work[...], proj_two, 0, 0)
    x_out[...] = dot_f32(inv_one[...], back, 1, 0)
    for lo in range(0, n, BLK):
        hi = lo + BLK
        if lo:
            r_out[lo:hi, :lo] = jnp.zeros((BLK, lo), jnp.float32)
        r_out[lo:hi, lo:] = dot_f32(r_two[lo:hi, lo:], r_one[lo:, lo:], 1, 0)


def finish(packed, r_one, inv_one, n_rhs):
    n = r_one.shape[0]
    return pl.pallas_call(
        finish_kernel,
        out_shape=[jax.ShapeDtypeStruct((n, n_rhs), jnp.float32), jax.ShapeDtypeStruct((n, n), jnp.float32)],
        in_specs=[pl.BlockSpec(memory_space=pltpu.VMEM)] * 3,
        out_specs=[pl.BlockSpec(memory_space=pltpu.VMEM)] * 2,
        scratch_shapes=[pltpu.VMEM((n, n), jnp.float32)] * 2,
        name="finish",
    )(packed, r_one, inv_one)


def solution(mesh):
    members = mesh.shape["rows"]

    def group_solve(a_blk, b_blk):
        n, n_rhs = a_blk.shape[1], b_blk.shape[1]
        gram_one = sum_over_rows(local_gram(a_blk, packed_rows(n, 0, members)), members, 1)
        r_one, inv_one = factor_one(gram_one, n)
        gram_two = sum_over_rows(local_basis(a_blk, b_blk, inv_one, packed_rows(n, n_rhs, members)), members, 2)
        return finish(gram_two, r_one, inv_one, n_rhs)

    row_spec = P(("batch", "rows"), None)
    out_spec = P("batch", None)
    return jax.shard_map(group_solve, mesh=mesh, in_specs=(row_spec, row_spec), out_specs=(out_spec, out_spec), check_vma=False)
```

```python
import functools
import jax
import jax.numpy as jnp
from jax import lax
from jax.experimental import pallas as pl
from jax.experimental.pallas import tpu as pltpu
from jax.sharding import PartitionSpec as P

HIGHEST = lax.Precision.HIGHEST
MESH = pl.DeviceIdType.MESH
LEAF = 8
BLK = 128
ROW_TILE = 512
VMEM_BYTES = 64000 * 1024


def dot_f32(lhs, rhs, lhs_dim, rhs_dim):
    return lax.dot_general(lhs, rhs, (((lhs_dim,), (rhs_dim,)), ((), ())), precision=HIGHEST, preferred_element_type=jnp.float32)


class RowSum:
    def __init__(self, members, sizes, part, out, pair_buf, acc, slots, sems):
        self.chips = members // 2
        me = lax.axis_index("rows")
        self.core, self.chip = lax.rem(me, 2), lax.div(me, 2)
        self.sizes = sizes
        self.starts = [sum(sizes[:g]) for g in range(len(sizes))]
        self.part, self.out, self.pair_buf, self.acc, self.slots = part, out, pair_buf, acc, slots
        self.swap_send, self.swap_recv, self.send, self.recv, self.back_send, self.back_recv, self.fwd_send, self.fwd_recv = sems

    def peer(self, d):
        return lax.rem(self.chip + d, self.chips)

    def pair_id(self):
        return {"rows": self.chip * 2 + 1 - self.core}

    def peer_id(self, d):
        return {"rows": self.peer(d) * 2 + self.core}

    def greet(self):
        barrier = pltpu.get_barrier_semaphore()
        pl.semaphore_signal(barrier, inc=1, device_id=self.pair_id(), device_id_type=MESH)
        for d in range(1, self.chips):
            pl.semaphore_signal(barrier, inc=1, device_id=self.peer_id(d), device_id_type=MESH)

    def await_all(self):
        pl.semaphore_wait(pltpu.get_barrier_semaphore(), self.chips)

    def half_rows(self, g, core):
        half = self.sizes[g] * BLK // 2
        return pl.ds(pl.multiple_of(self.starts[g] * BLK + core * half, 8), half)

    def chunk_of(self, g):
        return self.sizes[g] * BLK // (2 * self.chips)

    def own_rows(self, g, chip):
        half, chunk = self.sizes[g] * BLK // 2, self.chunk_of(g)
        return pl.ds(pl.multiple_of(self.starts[g] * BLK + self.core * half + chip * chunk, 8), chunk)

    def local_rows(self, g, chip):
        chunk = self.chunk_of(g)
        return pl.ds(pl.multiple_of(self.starts[g] * BLK // 2 + chip * chunk, 8), chunk)

    def local_half(self, g):
        return pl.ds(self.starts[g] * BLK // 2, self.sizes[g] * BLK // 2)

    def slot(self, g, d):
        chunk = self.chunk_of(g)
        base = self.starts[g] * BLK // (2 * self.chips)
        return self.slots.at[d - 1, pl.ds(base, chunk)]

    def swap(self, g):
        return pltpu.make_async_remote_copy(
            src_ref=self.part.at[self.half_rows(g, 1 - self.core)], dst_ref=self.pair_buf.at[self.local_half(g)],
            send_sem=self.swap_send.at[g], recv_sem=self.swap_recv.at[g], device_id=self.pair_id(), device_id_type=MESH)

    def scatter(self, g, d):
        return pltpu.make_async_remote_copy(
            src_ref=self.acc.at[self.local_rows(g, self.peer(d))], dst_ref=self.slot(g, d),
            send_sem=self.send.at[g, d - 1], recv_sem=self.recv.at[g, d - 1], device_id=self.peer_id(d), device_id_type=MESH)

    def gather(self, g, d):
        own = self.own_rows(g, self.chip)
        return pltpu.make_async_remote_copy(
            src_ref=self.out.at[own], dst_ref=self.out.at[own],
            send_sem=self.back_send.at[g, d - 1], recv_sem=self.back_recv.at[g, d - 1], device_id=self.peer_id(d), device_id_type=MESH)

    def forward(self, g, d):
        src = self.own_rows(g, self.peer(self.chips - d))
        return pltpu.make_async_remote_copy(
            src_ref=self.out.at[src], dst_ref=self.out.at[src],
            send_sem=self.fwd_send.at[g, d], recv_sem=self.fwd_recv.at[g, d], device_id=self.pair_id(), device_id_type=MESH)

    def start_swap(self, g):
        self.swap(g).start()

    def start_scatter(self, g):
        self.swap(g).wait()
        self.acc[self.local_half(g), :] = self.part[self.half_rows(g, self.core), :] + self.pair_buf[self.local_half(g), :]
        for d in range(1, self.chips):
            self.scatter(g, d).start()

    def start_gather(self, g):
        for d in range(1, self.chips):
            self.scatter(g, d).wait()
        total = self.acc[self.local_rows(g, self.chip), :]
        for d in range(1, self.chips):
            total = total + self.slot(g, d)[...]
        self.out[self.own_rows(g, self.chip), :] = total
        for d in range(1, self.chips):
            self.gather(g, d).start()
        self.forward(g, 0).start()

    def start_forward(self, g):
        for d in range(1, self.chips):
            self.gather(g, d).wait()
            self.forward(g, d).start()

    def drain(self, g):
        for d in range(self.chips):
            self.forward(g, d).wait()


def sum_scratch(members, sizes):
    chips = members // 2
    rows = sum(sizes) * BLK
    groups = len(sizes)
    sems = pltpu.SemaphoreType.DMA
    return [
        pltpu.VMEM((rows, BLK), jnp.float32), pltpu.VMEM((rows // 2, BLK), jnp.float32), pltpu.VMEM((rows // 2, BLK), jnp.float32),
        pltpu.VMEM((chips - 1, rows // (2 * chips), BLK), jnp.float32),
        sems((groups,)), sems((groups,)), sems((groups, chips - 1)), sems((groups, chips - 1)),
        sems((groups, chips - 1)), sems((groups, chips - 1)), sems((groups, chips)), sems((groups, chips)),
    ]


GRAM_GROUPS = (
    ((0, 2), (0, 3), (1, 2), (1, 3), (2, 2), (2, 3), (3, 3), (4, 2), (4, 3)),
    ((0, 0), (0, 1), (1, 1), (4, 0), (4, 1)),
    ((4, 4),),
)
BASIS_GROUPS = (
    ((0, 4), (1, 4), (2, 4), (3, 4), (4, 4)),
    ((0, 2), (0, 3), (1, 2), (1, 3), (2, 2), (2, 3), (3, 3)),
    ((0, 0), (0, 1), (1, 1)),
)


def proj_blocks(n):
    return -(-(n // 2) // BLK)


def block(idx):
    return slice(idx * BLK, (idx + 1) * BLK)


def pack_group(acc, part, start, pairs):
    for pos, (i, j) in enumerate(pairs):
        part[block(start + pos), :] = acc[block(i), block(j)] if i <= j else acc[block(i), block(j)].T


def tile_copy(src, dst, sem, t):
    rows = pl.ds(pl.multiple_of(t * ROW_TILE, ROW_TILE), ROW_TILE)
    return pltpu.make_async_copy(src.at[rows], dst.at[rows], sem.at[t])


def tile_rows(t):
    return pl.ds(pl.multiple_of(t * ROW_TILE, ROW_TILE), ROW_TILE)


def gram_kernel(members, a_hbm, out, a_buf, acc, load_sem, part, pair_buf, acc_half, slots, *sems):
    tiles = a_buf.shape[0] // ROW_TILE
    sizes = [len(group) for group in GRAM_GROUPS]
    total = RowSum(members, sizes, part, out, pair_buf, acc_half, slots, sems)
    total.greet()
    for t in range(tiles):
        tile_copy(a_hbm, a_buf, load_sem, t).start()
    acc[...] = jnp.zeros_like(acc)

    def first(t, carry):
        tile_copy(a_hbm, a_buf, load_sem, t).wait()
        rows = tile_rows(t)
        acc[:, 2 * BLK:4 * BLK] += dot_f32(a_buf[rows, :], a_buf[rows, 2 * BLK:4 * BLK], 0, 0)
        return carry

    lax.fori_loop(0, tiles, first, 0)
    pack_group(acc, part, total.starts[0], GRAM_GROUPS[0])
    total.await_all()
    total.start_swap(0)

    def second(t, carry):
        @pl.when(t == tiles // 4)
        def _():
            total.start_scatter(0)

        rows = tile_rows(t)
        rhs = a_buf[rows, :2 * BLK]
        acc[:2 * BLK, :2 * BLK] += dot_f32(rhs, rhs, 0, 0)
        acc[4 * BLK:, :2 * BLK] += dot_f32(a_buf[rows, 4 * BLK:], rhs, 0, 0)
        return carry

    lax.fori_loop(0, tiles, second, 0)
    pack_group(acc, part, total.starts[1], GRAM_GROUPS[1])
    total.start_swap(1)

    def third(t, carry):
        @pl.when(t == tiles // 4)
        def _():
            total.start_gather(0)

        @pl.when(t == tiles // 2)
        def _():
            total.start_scatter(1)

        last = a_buf[tile_rows(t), 4 * BLK:]
        acc[4 * BLK:, 4 * BLK:] += dot_f32(last, last, 0, 0)
        return carry

    lax.fori_loop(0, tiles, third, 0)
    pack_group(acc, part, total.starts[2], GRAM_GROUPS[2])
    total.start_swap(2)
    total.start_scatter(2)
    total.start_gather(1)
    total.start_forward(0)
    total.start_gather(2)
    total.start_forward(1)
    total.start_forward(2)
    for g in range(3):
        total.drain(g)


def gram_sum(a_blk, members, collective_id):
    m, n = a_blk.shape
    sizes = [len(group) for group in GRAM_GROUPS]
    return pl.pallas_call(
        functools.partial(gram_kernel, members),
        out_shape=jax.ShapeDtypeStruct((sum(sizes) * BLK, BLK), jnp.float32),
        in_specs=[pl.BlockSpec(memory_space=pl.ANY)],
        out_specs=pl.BlockSpec(memory_space=pltpu.VMEM),
        scratch_shapes=[pltpu.VMEM((m, n), jnp.float32), pltpu.VMEM((n, n), jnp.float32), pltpu.SemaphoreType.DMA((m // ROW_TILE,))] + sum_scratch(members, sizes),
        compiler_params=pltpu.CompilerParams(vmem_limit_bytes=VMEM_BYTES, collective_id=collective_id, has_side_effects=True),
        cost_estimate=pl.CostEstimate(flops=m * n * n * 6, bytes_accessed=4 * m * n, transcendentals=0),
        name="gram_one_sum",
    )(a_blk)


def basis_tile(a, inv, diag):
    left = dot_f32(a[:, :2 * BLK], inv[:2 * BLK, :2 * BLK], 1, 0)
    right = dot_f32(a[:, :4 * BLK], inv[:4 * BLK, 3 * BLK:], 1, 0)
    middle = dot_f32(a[:, :2 * BLK], inv[:2 * BLK, 2 * BLK:3 * BLK], 1, 0)
    ends = dot_f32(jnp.concatenate([a[:, 2 * BLK:3 * BLK], a[:, 4 * BLK:]], axis=1), diag[...], 1, 0)
    return left, middle + ends[:, :BLK], right[:, :BLK], right[:, BLK:] + ends[:, BLK:]


def basis_kernel(members, a_hbm, b_hbm, inv, out, a_buf, b_buf, diag, acc, acc_end, load_sem, b_sem, part, pair_buf, acc_half, slots, *sems):
    tiles = a_buf.shape[0] // ROW_TILE
    n, n_rhs = a_buf.shape[1], b_buf.shape[0]
    sizes = [len(group) for group in BASIS_GROUPS]
    n_end = sizes[0]
    sizes[0] += proj_blocks(n)
    total = RowSum(members, sizes, part, out, pair_buf, acc_half, slots, sems)
    total.greet()
    tile_copy(a_hbm, a_buf, load_sem, 0).start()
    b_copy = pltpu.make_async_copy(b_hbm, b_buf, b_sem)
    b_copy.start()
    for t in range(1, tiles):
        tile_copy(a_hbm, a_buf, load_sem, t).start()
    acc[...] = jnp.zeros_like(acc)
    acc_end[...] = jnp.zeros_like(acc_end)
    diag[...] = jnp.zeros_like(diag)
    diag[:BLK, :BLK] = inv[2 * BLK:3 * BLK, 2 * BLK:3 * BLK]
    diag[BLK:, BLK:] = inv[4 * BLK:, 4 * BLK:]
    b_copy.wait()

    def first(t, carry):
        tile_copy(a_hbm, a_buf, load_sem, t).wait()
        rows = tile_rows(t)
        left, third, fourth, fifth = basis_tile(a_buf[rows, :], inv, diag)
        a_buf[rows, :2 * BLK] = left
        a_buf[rows, 2 * BLK:3 * BLK] = third
        a_buf[rows, 3 * BLK:4 * BLK] = fourth
        a_buf[rows, 4 * BLK:] = fifth
        both = jnp.concatenate([fifth, b_buf[:, tile_rows(t)].T], axis=1)
        acc_end[...] += dot_f32(a_buf[rows, :], both, 0, 0)
        return carry

    lax.fori_loop(0, tiles, first, 0)
    for pos, (i, _) in enumerate(BASIS_GROUPS[0]):
        part[block(pos), :] = acc_end[block(i), :BLK]
    half = n // 2
    base = n_end * BLK
    part[base:base + half, :] = jnp.concatenate([acc_end[:half, BLK:], acc_end[half:, BLK:]], axis=1)
    if base + half < sizes[0] * BLK:
        part[base + half:sizes[0] * BLK, :] = jnp.zeros((sizes[0] * BLK - base - half, BLK), jnp.float32)
    total.await_all()
    total.start_swap(0)

    def second(t, carry):
        @pl.when(t == tiles // 4)
        def _():
            total.start_scatter(0)

        rows = tile_rows(t)
        acc[:, 2 * BLK:] += dot_f32(a_buf[rows, :4 * BLK], a_buf[rows, 2 * BLK:4 * BLK], 0, 0)
        return carry

    lax.fori_loop(0, tiles, second, 0)
    pack_group(acc, part, total.starts[1], BASIS_GROUPS[1])
    total.start_swap(1)
    total.start_gather(0)

    def third_part(t, carry):
        @pl.when(t == tiles // 4)
        def _():
            total.start_scatter(1)

        rows = tile_rows(t)
        rhs = a_buf[rows, :2 * BLK]
        acc[:2 * BLK, :2 * BLK] += dot_f32(rhs, rhs, 0, 0)
        return carry

    lax.fori_loop(0, tiles, third_part, 0)
    pack_group(acc, part, total.starts[2], BASIS_GROUPS[2])
    total.start_swap(2)
    total.start_scatter(2)
    total.start_forward(0)
    total.start_gather(1)
    total.start_gather(2)
    total.start_forward(1)
    total.start_forward(2)
    for g in range(3):
        total.drain(g)


def basis_sum(a_blk, b_blk, r_inv, members, collective_id):
    m, n = a_blk.shape
    n_rhs = b_blk.shape[1]
    sizes = [len(group) for group in BASIS_GROUPS]
    sizes[0] += proj_blocks(n)
    any_spec, vmem_spec = pl.BlockSpec(memory_space=pl.ANY), pl.BlockSpec(memory_space=pltpu.VMEM)
    return pl.pallas_call(
        functools.partial(basis_kernel, members),
        out_shape=jax.ShapeDtypeStruct((sum(sizes) * BLK, BLK), jnp.float32),
        in_specs=[any_spec, any_spec, vmem_spec],
        out_specs=vmem_spec,
        scratch_shapes=[
            pltpu.VMEM((m, n), jnp.float32), pltpu.VMEM((n_rhs, m), jnp.float32), pltpu.VMEM((2 * BLK, 2 * BLK), jnp.float32),
            pltpu.VMEM((4 * BLK, 4 * BLK), jnp.float32), pltpu.VMEM((n, BLK + n_rhs), jnp.float32),
            pltpu.SemaphoreType.DMA((m // ROW_TILE,)), pltpu.SemaphoreType.DMA,
        ] + sum_scratch(members, sizes),
        compiler_params=pltpu.CompilerParams(vmem_limit_bytes=VMEM_BYTES, collective_id=collective_id, has_side_effects=True),
        cost_estimate=pl.CostEstimate(flops=m * n * n * 12, bytes_accessed=4 * m * (n + n_rhs), transcendentals=0),
        name="basis_gram_two_sum",
    )(a_blk, b_blk.T, r_inv)


def row_of(arr, idx):
    return jnp.broadcast_to(arr[idx:idx + 1, :], (LEAF, arr.shape[1]))


def factor_block(sym):
    n_leaf = BLK // LEAF
    ahead = 2
    row_id = lax.broadcasted_iota(jnp.int32, (BLK, BLK), 0)
    col_id = lax.broadcasted_iota(jnp.int32, (BLK, BLK), 1)
    eye = (row_id == col_id).astype(jnp.float32)
    sub_id = lax.broadcasted_iota(jnp.int32, (LEAF, BLK), 0)
    s_rows = [sym[LEAF * t:LEAF * (t + 1), :] for t in range(n_leaf)]
    i_rows = [eye[LEAF * t:LEAF * (t + 1), :] for t in range(n_leaf)]
    for t in range(n_leaf):
        span = list(range(t, min(t + ahead + 1, n_leaf)))
        ecol = [[jnp.broadcast_to(s_rows[u][:, LEAF * t + i:LEAF * t + i + 1], (LEAF, BLK)) for u in span] for i in range(LEAF)]
        w_s, w_i = s_rows[t], i_rows[t]
        for i in range(LEAF):
            inv = lax.rsqrt(row_of(ecol[i][0], i))
            lcol = [e * inv for e in ecol[i]]
            bc_s = row_of(s_rows[t], i) * inv
            bc_i = row_of(i_rows[t], i) * inv
            w_s = jnp.where(sub_id == i, bc_s, w_s)
            w_i = jnp.where(sub_id == i, bc_i, w_i)
            for v, u in enumerate(span):
                if v == 0 and i == LEAF - 1:
                    continue
                s_rows[u] = s_rows[u] - lcol[v] * bc_s
                i_next = i_rows[u] - lcol[v] * bc_i
                i_rows[u] = i_next if v else jnp.where(sub_id > i, i_next, i_rows[u])
            for j in range(i + 1, LEAF):
                piv = row_of(lcol[0], j)
                ecol[j] = [e - c * piv for e, c in zip(ecol[j], lcol)]
        s_rows[t], i_rows[t] = w_s, w_i
        rest = t + ahead + 1
        if rest < n_leaf:
            upd = dot_f32(w_s, jnp.concatenate([w_s, w_i], axis=1), 0, 0)
            for u in range(rest, n_leaf):
                s_rows[u] = s_rows[u] - upd[LEAF * u:LEAF * (u + 1), :BLK]
                i_rows[u] = i_rows[u] - upd[LEAF * u:LEAF * (u + 1), BLK:]
    r_blk = jnp.where(row_id <= col_id, jnp.concatenate(s_rows, axis=0), 0.0)
    linv = jnp.where(row_id >= col_id, jnp.concatenate(i_rows, axis=0), 0.0)
    return r_blk, linv


def factor_all(work, r_out, n):
    n_blk = n // BLK

    def step(k, carry):
        base = pl.multiple_of(k * BLK, BLK)
        r_blk, linv = factor_block(work[pl.ds(base, BLK), pl.ds(base, BLK)])
        for kk in range(n_blk):
            @pl.when(k == kk)
            def _():
                lo, hi = BLK * kk, BLK * (kk + 1)
                if lo:
                    work[lo:hi, :lo] = dot_f32(linv, work[lo:hi, :lo], 1, 0)
                    r_out[lo:hi, :lo] = jnp.zeros((BLK, lo), jnp.float32)
                work[lo:hi, lo:hi] = linv
                r_out[lo:hi, lo:hi] = r_blk
                if hi < n:
                    r_row = dot_f32(linv, work[lo:hi, hi:], 1, 0)
                    r_out[lo:hi, hi:] = r_row
                    work[lo:hi, hi:] = jnp.zeros((BLK, n - hi), jnp.float32)
                    for ii in range(kk + 1, n_blk):
                        a, b = BLK * ii, BLK * (ii + 1)
                        fac = r_row[:, a - hi:b - hi]
                        work[a:b, a:] = work[a:b, a:] - dot_f32(fac, r_row[:, a - hi:], 0, 0)
                        if lo:
                            work[a:b, :lo] = work[a:b, :lo] - dot_f32(fac, work[lo:hi, :lo], 0, 0)
                        work[a:b, lo:hi] = -dot_f32(fac, linv, 0, 0)
        return carry

    lax.fori_loop(0, n_blk, step, 0)


def unpack_upper(packed, work, groups, skip):
    start = 0
    for group in groups:
        for pos, (i, j) in enumerate(group):
            lo, hi = min(i, j), max(i, j)
            work[block(lo), block(hi)] = packed[block(start + pos), :]
        start += len(group) + (skip if group is groups[0] else 0)


def factor_kernel(packed, r_out, inv_out, work):
    n = work.shape[0]
    unpack_upper(packed, work, GRAM_GROUPS, 0)
    factor_all(work, r_out, n)
    for c in range(0, n, BLK):
        inv_out[:, c:c + BLK] = work[c:c + BLK, :].T


def factor_one(packed, n):
    return pl.pallas_call(
        factor_kernel,
        out_shape=[jax.ShapeDtypeStruct((n, n), jnp.float32)] * 2,
        in_specs=[pl.BlockSpec(memory_space=pltpu.VMEM)],
        out_specs=[pl.BlockSpec(memory_space=pltpu.VMEM)] * 2,
        scratch_shapes=[pltpu.VMEM((n, n), jnp.float32)],
        name="factor_one",
    )(packed)


def finish_kernel(packed, r_one, inv_one, x_out, r_out, work, r_two):
    n_rhs, n = x_out.shape
    unpack_upper(packed, work, BASIS_GROUPS, proj_blocks(n))
    factor_all(work, r_two, n)
    base = len(BASIS_GROUPS[0]) * BLK
    half = n // 2
    flat = packed[base:base + half, :]
    proj = jnp.concatenate([flat[:, :n_rhs], flat[:, n_rhs:]], axis=0)
    proj_two = dot_f32(work[...], proj, 1, 0)
    back = dot_f32(work[...], proj_two, 0, 0)
    x_out[...] = dot_f32(inv_one[...], back, 1, 0).T
    for lo in range(0, n, BLK):
        hi = lo + BLK
        if lo:
            r_out[lo:hi, :lo] = jnp.zeros((BLK, lo), jnp.float32)
        r_out[lo:hi, lo:] = dot_f32(r_two[lo:hi, lo:], r_one[lo:, lo:], 1, 0)


def finish(packed, r_one, inv_one, n_rhs):
    n = r_one.shape[0]
    return pl.pallas_call(
        finish_kernel,
        out_shape=[jax.ShapeDtypeStruct((n_rhs, n), jnp.float32), jax.ShapeDtypeStruct((n, n), jnp.float32)],
        in_specs=[pl.BlockSpec(memory_space=pltpu.VMEM)] * 3,
        out_specs=[pl.BlockSpec(memory_space=pltpu.VMEM)] * 2,
        scratch_shapes=[pltpu.VMEM((n, n), jnp.float32)] * 2,
        name="finish",
    )(packed, r_one, inv_one)


def solution(mesh):
    members = mesh.shape["rows"]

    def group_solve(a_blk, b_blk):
        n, n_rhs = a_blk.shape[1], b_blk.shape[1]
        gram_one = gram_sum(a_blk, members, 1)
        r_one, inv_one = factor_one(gram_one, n)
        gram_two = basis_sum(a_blk, b_blk, inv_one, members, 2)
        x_flat, r_factor = finish(gram_two, r_one, inv_one, n_rhs)
        return x_flat.T, r_factor

    row_spec = P(("batch", "rows"), None)
    out_spec = P("batch", None)
    return jax.shard_map(group_solve, mesh=mesh, in_specs=(row_spec, row_spec), out_specs=(out_spec, out_spec), check_vma=False)
```

```python
import functools
import jax
import jax.numpy as jnp
from jax import lax
from jax.experimental import pallas as pl
from jax.experimental.pallas import tpu as pltpu
from jax.sharding import PartitionSpec as P

HIGHEST = lax.Precision.HIGHEST
MESH = pl.DeviceIdType.MESH
LEAF = 8
GROUP = 2
AHEAD = 2
BLK = 128
GRAM_TILES = (512, 1024, 1024)
BASIS_TILES = (512, 1024, 1024)
VMEM_BYTES = 64000 * 1024


def dot_f32(lhs, rhs, lhs_dim, rhs_dim):
    return lax.dot_general(lhs, rhs, (((lhs_dim,), (rhs_dim,)), ((), ())), precision=HIGHEST, preferred_element_type=jnp.float32)


class RowSum:
    def __init__(self, members, sizes, part, out, pair_buf, acc, slots, sems):
        self.chips = members // 2
        me = lax.axis_index("rows")
        self.core, self.chip = lax.rem(me, 2), lax.div(me, 2)
        self.sizes = sizes
        self.starts = [sum(sizes[:g]) for g in range(len(sizes))]
        self.part, self.out, self.pair_buf, self.acc, self.slots = part, out, pair_buf, acc, slots
        self.swap_send, self.swap_recv, self.send, self.recv, self.back_send, self.back_recv, self.fwd_send, self.fwd_recv = sems

    def peer(self, d):
        return lax.rem(self.chip + d, self.chips)

    def pair_id(self):
        return {"rows": self.chip * 2 + 1 - self.core}

    def peer_id(self, d):
        return {"rows": self.peer(d) * 2 + self.core}

    def greet(self):
        barrier = pltpu.get_barrier_semaphore()
        pl.semaphore_signal(barrier, inc=1, device_id=self.pair_id(), device_id_type=MESH)
        for d in range(1, self.chips):
            pl.semaphore_signal(barrier, inc=1, device_id=self.peer_id(d), device_id_type=MESH)

    def await_all(self):
        pl.semaphore_wait(pltpu.get_barrier_semaphore(), self.chips)

    def half_rows(self, g, core):
        half = self.sizes[g] * BLK // 2
        return pl.ds(pl.multiple_of(self.starts[g] * BLK + core * half, 8), half)

    def chunk_of(self, g):
        return self.sizes[g] * BLK // (2 * self.chips)

    def own_rows(self, g, chip):
        half, chunk = self.sizes[g] * BLK // 2, self.chunk_of(g)
        return pl.ds(pl.multiple_of(self.starts[g] * BLK + self.core * half + chip * chunk, 8), chunk)

    def local_rows(self, g, chip):
        chunk = self.chunk_of(g)
        return pl.ds(pl.multiple_of(self.starts[g] * BLK // 2 + chip * chunk, 8), chunk)

    def local_half(self, g):
        return pl.ds(self.starts[g] * BLK // 2, self.sizes[g] * BLK // 2)

    def slot(self, g, d):
        chunk = self.chunk_of(g)
        base = self.starts[g] * BLK // (2 * self.chips)
        return self.slots.at[d - 1, pl.ds(base, chunk)]

    def swap(self, g):
        return pltpu.make_async_remote_copy(
            src_ref=self.part.at[self.half_rows(g, 1 - self.core)], dst_ref=self.pair_buf.at[self.local_half(g)],
            send_sem=self.swap_send.at[g], recv_sem=self.swap_recv.at[g], device_id=self.pair_id(), device_id_type=MESH)

    def scatter(self, g, d):
        return pltpu.make_async_remote_copy(
            src_ref=self.acc.at[self.local_rows(g, self.peer(d))], dst_ref=self.slot(g, d),
            send_sem=self.send.at[g, d - 1], recv_sem=self.recv.at[g, d - 1], device_id=self.peer_id(d), device_id_type=MESH)

    def gather(self, g, d):
        own = self.own_rows(g, self.chip)
        return pltpu.make_async_remote_copy(
            src_ref=self.out.at[own], dst_ref=self.out.at[own],
            send_sem=self.back_send.at[g, d - 1], recv_sem=self.back_recv.at[g, d - 1], device_id=self.peer_id(d), device_id_type=MESH)

    def forward(self, g, d):
        src = self.own_rows(g, self.peer(self.chips - d))
        return pltpu.make_async_remote_copy(
            src_ref=self.out.at[src], dst_ref=self.out.at[src],
            send_sem=self.fwd_send.at[g, d], recv_sem=self.fwd_recv.at[g, d], device_id=self.pair_id(), device_id_type=MESH)

    def start_swap(self, g):
        self.swap(g).start()

    def start_scatter(self, g):
        self.swap(g).wait()
        self.acc[self.local_half(g), :] = self.part[self.half_rows(g, self.core), :] + self.pair_buf[self.local_half(g), :]
        for d in range(1, self.chips):
            self.scatter(g, d).start()

    def start_gather(self, g):
        for d in range(1, self.chips):
            self.scatter(g, d).wait()
        total = self.acc[self.local_rows(g, self.chip), :]
        for d in range(1, self.chips):
            total = total + self.slot(g, d)[...]
        self.out[self.own_rows(g, self.chip), :] = total
        for d in range(1, self.chips):
            self.gather(g, d).start()
        self.forward(g, 0).start()

    def start_forward(self, g):
        for d in range(1, self.chips):
            self.gather(g, d).wait()
            self.forward(g, d).start()

    def drain(self, g):
        for d in range(self.chips):
            self.forward(g, d).wait()


def sum_scratch(members, sizes):
    chips = members // 2
    rows = sum(sizes) * BLK
    groups = len(sizes)
    sems = pltpu.SemaphoreType.DMA
    return [
        pltpu.VMEM((rows, BLK), jnp.float32), pltpu.VMEM((rows // 2, BLK), jnp.float32), pltpu.VMEM((rows // 2, BLK), jnp.float32),
        pltpu.VMEM((chips - 1, rows // (2 * chips), BLK), jnp.float32),
        sems((groups,)), sems((groups,)), sems((groups, chips - 1)), sems((groups, chips - 1)),
        sems((groups, chips - 1)), sems((groups, chips - 1)), sems((groups, chips)), sems((groups, chips)),
    ]


GRAM_GROUPS = (
    ((0, 2), (0, 3), (1, 2), (1, 3), (2, 2), (2, 3), (3, 3), (4, 2), (4, 3)),
    ((0, 0), (0, 1), (1, 1), (4, 0), (4, 1)),
    ((4, 4),),
)
BASIS_GROUPS = (
    ((0, 4), (1, 4), (2, 4), (3, 4), (4, 4)),
    ((0, 2), (0, 3), (1, 2), (1, 3), (2, 2), (2, 3), (3, 3)),
    ((0, 0), (0, 1), (1, 1)),
)


def proj_blocks(n):
    return -(-(n // 2) // BLK)


def block(idx):
    return slice(idx * BLK, (idx + 1) * BLK)


def pack_group(acc, part, start, pairs):
    for pos, (i, j) in enumerate(pairs):
        part[block(start + pos), :] = acc[block(i), block(j)] if i <= j else acc[block(i), block(j)].T


def tile_rows(t, size):
    return pl.ds(pl.multiple_of(t * size, size), size)


def tile_copy(src, dst, sem, t, size):
    rows = tile_rows(t, size)
    return pltpu.make_async_copy(src.at[rows], dst.at[rows], sem.at[t])


def gram_kernel(members, a_hbm, out, a_buf, acc, load_sem, part, pair_buf, acc_half, slots, *sems):
    first_size, second_size, third_size = GRAM_TILES
    tiles = a_buf.shape[0] // first_size
    sizes = [len(group) for group in GRAM_GROUPS]
    total = RowSum(members, sizes, part, out, pair_buf, acc_half, slots, sems)
    total.greet()
    for t in range(tiles):
        tile_copy(a_hbm, a_buf, load_sem, t, first_size).start()
    acc[...] = jnp.zeros_like(acc)

    def first(t, carry):
        tile_copy(a_hbm, a_buf, load_sem, t, first_size).wait()
        rows = tile_rows(t, first_size)
        acc[:, 2 * BLK:4 * BLK] += dot_f32(a_buf[rows, :], a_buf[rows, 2 * BLK:4 * BLK], 0, 0)
        return carry

    lax.fori_loop(0, tiles, first, 0)
    pack_group(acc, part, total.starts[0], GRAM_GROUPS[0])
    total.await_all()
    total.start_swap(0)

    def second(t, carry):
        @pl.when(t == 1)
        def _():
            total.start_scatter(0)

        rows = tile_rows(t, second_size)
        rhs = a_buf[rows, :2 * BLK]
        acc[:2 * BLK, :2 * BLK] += dot_f32(rhs, rhs, 0, 0)
        acc[4 * BLK:, :2 * BLK] += dot_f32(a_buf[rows, 4 * BLK:], rhs, 0, 0)
        return carry

    lax.fori_loop(0, a_buf.shape[0] // second_size, second, 0)
    pack_group(acc, part, total.starts[1], GRAM_GROUPS[1])
    total.start_swap(1)

    def third(t, carry):
        @pl.when(t == 0)
        def _():
            total.start_gather(0)

        @pl.when(t == 3)
        def _():
            total.start_scatter(1)

        last = a_buf[tile_rows(t, third_size), 4 * BLK:]
        acc[4 * BLK:, 4 * BLK:] += dot_f32(last, last, 0, 0)
        return carry

    lax.fori_loop(0, a_buf.shape[0] // third_size, third, 0)
    pack_group(acc, part, total.starts[2], GRAM_GROUPS[2])
    total.start_swap(2)
    total.start_scatter(2)
    total.start_gather(1)
    total.start_forward(0)
    total.start_gather(2)
    total.start_forward(1)
    total.start_forward(2)
    for g in range(3):
        total.drain(g)


def gram_sum(a_blk, members, collective_id):
    m, n = a_blk.shape
    sizes = [len(group) for group in GRAM_GROUPS]
    return pl.pallas_call(
        functools.partial(gram_kernel, members),
        out_shape=jax.ShapeDtypeStruct((sum(sizes) * BLK, BLK), jnp.float32),
        in_specs=[pl.BlockSpec(memory_space=pl.ANY)],
        out_specs=pl.BlockSpec(memory_space=pltpu.VMEM),
        scratch_shapes=[pltpu.VMEM((m, n), jnp.float32), pltpu.VMEM((n, n), jnp.float32), pltpu.SemaphoreType.DMA((m // GRAM_TILES[0],))] + sum_scratch(members, sizes),
        compiler_params=pltpu.CompilerParams(vmem_limit_bytes=VMEM_BYTES, collective_id=collective_id, has_side_effects=True),
        cost_estimate=pl.CostEstimate(flops=m * n * n * 6, bytes_accessed=4 * m * n, transcendentals=0),
        name="gram_one_sum",
    )(a_blk)


def basis_tile(a, inv, diag):
    left = dot_f32(a[:, :2 * BLK], inv[:2 * BLK, :2 * BLK], 1, 0)
    right = dot_f32(a[:, :4 * BLK], inv[:4 * BLK, 3 * BLK:], 1, 0)
    middle = dot_f32(a[:, :2 * BLK], inv[:2 * BLK, 2 * BLK:3 * BLK], 1, 0)
    ends = dot_f32(jnp.concatenate([a[:, 2 * BLK:3 * BLK], a[:, 4 * BLK:]], axis=1), diag[...], 1, 0)
    return left, middle + ends[:, :BLK], right[:, :BLK], right[:, BLK:] + ends[:, BLK:]


def basis_kernel(members, a_hbm, b_hbm, inv, out, a_buf, b_buf, diag, acc, acc_end, load_sem, b_sem, part, pair_buf, acc_half, slots, *sems):
    first_size, second_size, third_size = BASIS_TILES
    tiles = a_buf.shape[0] // first_size
    n, n_rhs = a_buf.shape[1], b_buf.shape[0]
    sizes = [len(group) for group in BASIS_GROUPS]
    n_end = sizes[0]
    sizes[0] += proj_blocks(n)
    total = RowSum(members, sizes, part, out, pair_buf, acc_half, slots, sems)
    total.greet()
    tile_copy(a_hbm, a_buf, load_sem, 0, first_size).start()
    b_copy = pltpu.make_async_copy(b_hbm, b_buf, b_sem)
    b_copy.start()
    for t in range(1, tiles):
        tile_copy(a_hbm, a_buf, load_sem, t, first_size).start()
    acc[...] = jnp.zeros_like(acc)
    acc_end[...] = jnp.zeros_like(acc_end)
    diag[...] = jnp.zeros_like(diag)
    diag[:BLK, :BLK] = inv[2 * BLK:3 * BLK, 2 * BLK:3 * BLK]
    diag[BLK:, BLK:] = inv[4 * BLK:, 4 * BLK:]
    b_copy.wait()

    def first(t, carry):
        tile_copy(a_hbm, a_buf, load_sem, t, first_size).wait()
        rows = tile_rows(t, first_size)
        left, third, fourth, fifth = basis_tile(a_buf[rows, :], inv, diag)
        a_buf[rows, :2 * BLK] = left
        a_buf[rows, 2 * BLK:3 * BLK] = third
        a_buf[rows, 3 * BLK:4 * BLK] = fourth
        a_buf[rows, 4 * BLK:] = fifth
        both = jnp.concatenate([fifth, b_buf[:, tile_rows(t, first_size)].T], axis=1)
        acc_end[...] += dot_f32(a_buf[rows, :], both, 0, 0)
        return carry

    lax.fori_loop(0, tiles, first, 0)
    for pos, (i, _) in enumerate(BASIS_GROUPS[0]):
        part[block(pos), :] = acc_end[block(i), :BLK]
    half = n // 2
    base = n_end * BLK
    part[base:base + half, :] = jnp.concatenate([acc_end[:half, BLK:], acc_end[half:, BLK:]], axis=1)
    if base + half < sizes[0] * BLK:
        part[base + half:sizes[0] * BLK, :] = jnp.zeros((sizes[0] * BLK - base - half, BLK), jnp.float32)
    total.await_all()
    total.start_swap(0)

    def second(t, carry):
        @pl.when(t == 1)
        def _():
            total.start_scatter(0)

        @pl.when(t == 6)
        def _():
            total.start_gather(0)

        rows = tile_rows(t, second_size)
        acc[:, 2 * BLK:] += dot_f32(a_buf[rows, :4 * BLK], a_buf[rows, 2 * BLK:4 * BLK], 0, 0)
        return carry

    lax.fori_loop(0, a_buf.shape[0] // second_size, second, 0)
    pack_group(acc, part, total.starts[1], BASIS_GROUPS[1])
    total.start_swap(1)

    def third_part(t, carry):
        @pl.when(t == 1)
        def _():
            total.start_scatter(1)

        rows = tile_rows(t, third_size)
        rhs = a_buf[rows, :2 * BLK]
        acc[:2 * BLK, :2 * BLK] += dot_f32(rhs, rhs, 0, 0)
        return carry

    lax.fori_loop(0, a_buf.shape[0] // third_size, third_part, 0)
    pack_group(acc, part, total.starts[2], BASIS_GROUPS[2])
    total.start_swap(2)
    total.start_scatter(2)
    total.start_forward(0)
    total.start_gather(1)
    total.start_gather(2)
    total.start_forward(1)
    total.start_forward(2)
    for g in range(3):
        total.drain(g)


def basis_sum(a_blk, b_blk, r_inv, members, collective_id):
    m, n = a_blk.shape
    n_rhs = b_blk.shape[1]
    sizes = [len(group) for group in BASIS_GROUPS]
    sizes[0] += proj_blocks(n)
    any_spec, vmem_spec = pl.BlockSpec(memory_space=pl.ANY), pl.BlockSpec(memory_space=pltpu.VMEM)
    return pl.pallas_call(
        functools.partial(basis_kernel, members),
        out_shape=jax.ShapeDtypeStruct((sum(sizes) * BLK, BLK), jnp.float32),
        in_specs=[any_spec, any_spec, vmem_spec],
        out_specs=vmem_spec,
        scratch_shapes=[
            pltpu.VMEM((m, n), jnp.float32), pltpu.VMEM((n_rhs, m), jnp.float32), pltpu.VMEM((2 * BLK, 2 * BLK), jnp.float32),
            pltpu.VMEM((4 * BLK, 4 * BLK), jnp.float32), pltpu.VMEM((n, BLK + n_rhs), jnp.float32),
            pltpu.SemaphoreType.DMA((m // BASIS_TILES[0],)), pltpu.SemaphoreType.DMA,
        ] + sum_scratch(members, sizes),
        compiler_params=pltpu.CompilerParams(vmem_limit_bytes=VMEM_BYTES, collective_id=collective_id, has_side_effects=True),
        cost_estimate=pl.CostEstimate(flops=m * n * n * 12, bytes_accessed=4 * m * (n + n_rhs), transcendentals=0),
        name="basis_gram_two_sum",
    )(a_blk, b_blk.T, r_inv)


def row_of(arr, idx):
    return jnp.broadcast_to(arr[idx:idx + 1, :], (LEAF, arr.shape[1]))


def factor_block(sym):
    n_leaf = BLK // LEAF
    row_id = lax.broadcasted_iota(jnp.int32, (BLK, BLK), 0)
    col_id = lax.broadcasted_iota(jnp.int32, (BLK, BLK), 1)
    eye = (row_id == col_id).astype(jnp.float32)
    sub_id = lax.broadcasted_iota(jnp.int32, (LEAF, BLK), 0)
    s_rows = [sym[LEAF * t:LEAF * (t + 1), :] for t in range(n_leaf)]
    i_rows = [eye[LEAF * t:LEAF * (t + 1), :] for t in range(n_leaf)]
    for t in range(0, n_leaf, GROUP):
        first = LEAF * t
        span = list(range(t, min(t + GROUP + AHEAD, n_leaf)))
        ecol = [[jnp.broadcast_to(s_rows[u][:, first + j:first + j + 1], (LEAF, BLK)) if u >= t + j // LEAF else None for u in span] for j in range(GROUP * LEAF)]
        done_s, done_i = list(s_rows[t:t + GROUP]), list(i_rows[t:t + GROUP])
        for i in range(GROUP * LEAF):
            v0, sub = i // LEAF, i % LEAF
            inv = lax.rsqrt(row_of(ecol[i][v0], sub))
            lcol = [None] * v0 + [e * inv for e in ecol[i][v0:]]
            bc_s = row_of(s_rows[t + v0], sub) * inv
            bc_i = row_of(i_rows[t + v0], sub) * inv
            done_s[v0] = jnp.where(sub_id == sub, bc_s, done_s[v0])
            done_i[v0] = jnp.where(sub_id == sub, bc_i, done_i[v0])
            for v in range(v0, len(span)):
                if v == v0 and sub == LEAF - 1:
                    continue
                u = span[v]
                s_rows[u] = s_rows[u] - lcol[v] * bc_s
                i_rows[u] = i_rows[u] - lcol[v] * bc_i
            for j in range(i + 1, GROUP * LEAF):
                piv = row_of(lcol[j // LEAF], j % LEAF)
                for v in range(j // LEAF, len(span)):
                    ecol[j][v] = ecol[j][v] - lcol[v] * piv
        s_rows[t:t + GROUP], i_rows[t:t + GROUP] = done_s, done_i
        rest = t + GROUP + AHEAD
        if rest < n_leaf:
            w_s = jnp.concatenate(done_s, axis=0)
            upd = dot_f32(w_s, jnp.concatenate([w_s, jnp.concatenate(done_i, axis=0)], axis=1), 0, 0)
            for u in range(rest, n_leaf):
                s_rows[u] = s_rows[u] - upd[LEAF * u:LEAF * (u + 1), :BLK]
                i_rows[u] = i_rows[u] - upd[LEAF * u:LEAF * (u + 1), BLK:]
    r_blk = jnp.where(row_id <= col_id, jnp.concatenate(s_rows, axis=0), 0.0)
    linv = jnp.where(row_id >= col_id, jnp.concatenate(i_rows, axis=0), 0.0)
    return r_blk, linv


def factor_all(work, r_out, n):
    n_blk = n // BLK

    def step(k, carry):
        base = pl.multiple_of(k * BLK, BLK)
        r_blk, linv = factor_block(work[pl.ds(base, BLK), pl.ds(base, BLK)])
        for kk in range(n_blk):
            @pl.when(k == kk)
            def _():
                lo, hi = BLK * kk, BLK * (kk + 1)
                if lo:
                    work[lo:hi, :lo] = dot_f32(linv, work[lo:hi, :lo], 1, 0)
                    r_out[lo:hi, :lo] = jnp.zeros((BLK, lo), jnp.float32)
                work[lo:hi, lo:hi] = linv
                r_out[lo:hi, lo:hi] = r_blk
                if hi < n:
                    r_row = dot_f32(linv, work[lo:hi, hi:], 1, 0)
                    r_out[lo:hi, hi:] = r_row
                    work[lo:hi, hi:] = jnp.zeros((BLK, n - hi), jnp.float32)
                    for ii in range(kk + 1, n_blk):
                        a, b = BLK * ii, BLK * (ii + 1)
                        fac = r_row[:, a - hi:b - hi]
                        work[a:b, a:] = work[a:b, a:] - dot_f32(fac, r_row[:, a - hi:], 0, 0)
                        if lo:
                            work[a:b, :lo] = work[a:b, :lo] - dot_f32(fac, work[lo:hi, :lo], 0, 0)
                        work[a:b, lo:hi] = -dot_f32(fac, linv, 0, 0)
        return carry

    lax.fori_loop(0, n_blk, step, 0)


def unpack_upper(packed, work, groups, skip):
    start = 0
    for group in groups:
        for pos, (i, j) in enumerate(group):
            lo, hi = min(i, j), max(i, j)
            work[block(lo), block(hi)] = packed[block(start + pos), :]
        start += len(group) + (skip if group is groups[0] else 0)


def factor_kernel(packed, r_out, inv_out, work):
    n = work.shape[0]
    unpack_upper(packed, work, GRAM_GROUPS, 0)
    factor_all(work, r_out, n)
    for c in range(0, n, BLK):
        inv_out[:, c:c + BLK] = work[c:c + BLK, :].T


def factor_one(packed, n):
    return pl.pallas_call(
        factor_kernel,
        out_shape=[jax.ShapeDtypeStruct((n, n), jnp.float32)] * 2,
        in_specs=[pl.BlockSpec(memory_space=pltpu.VMEM)],
        out_specs=[pl.BlockSpec(memory_space=pltpu.VMEM)] * 2,
        scratch_shapes=[pltpu.VMEM((n, n), jnp.float32)],
        name="factor_one",
    )(packed)


def finish_kernel(packed, r_one, inv_one, x_out, r_out, work, r_two):
    n_rhs, n = x_out.shape
    unpack_upper(packed, work, BASIS_GROUPS, proj_blocks(n))
    factor_all(work, r_two, n)
    base = len(BASIS_GROUPS[0]) * BLK
    half = n // 2
    flat = packed[base:base + half, :]
    proj = jnp.concatenate([flat[:, :n_rhs], flat[:, n_rhs:]], axis=0)
    proj_two = dot_f32(work[...], proj, 1, 0)
    back = dot_f32(work[...], proj_two, 0, 0)
    x_out[...] = dot_f32(inv_one[...], back, 1, 0).T
    for lo in range(0, n, BLK):
        hi = lo + BLK
        if lo:
            r_out[lo:hi, :lo] = jnp.zeros((BLK, lo), jnp.float32)
        r_out[lo:hi, lo:] = dot_f32(r_two[lo:hi, lo:], r_one[lo:, lo:], 1, 0)


def finish(packed, r_one, inv_one, n_rhs):
    n = r_one.shape[0]
    return pl.pallas_call(
        finish_kernel,
        out_shape=[jax.ShapeDtypeStruct((n_rhs, n), jnp.float32), jax.ShapeDtypeStruct((n, n), jnp.float32)],
        in_specs=[pl.BlockSpec(memory_space=pltpu.VMEM)] * 3,
        out_specs=[pl.BlockSpec(memory_space=pltpu.VMEM)] * 2,
        scratch_shapes=[pltpu.VMEM((n, n), jnp.float32)] * 2,
        name="finish",
    )(packed, r_one, inv_one)


def solution(mesh):
    members = mesh.shape["rows"]

    def group_solve(a_blk, b_blk):
        n, n_rhs = a_blk.shape[1], b_blk.shape[1]
        gram_one = gram_sum(a_blk, members, 1)
        r_one, inv_one = factor_one(gram_one, n)
        gram_two = basis_sum(a_blk, b_blk, inv_one, members, 2)
        x_flat, r_factor = finish(gram_two, r_one, inv_one, n_rhs)
        return x_flat.T, r_factor

    row_spec = P(("batch", "rows"), None)
    out_spec = P("batch", None)
    return jax.shard_map(group_solve, mesh=mesh, in_specs=(row_spec, row_spec), out_specs=(out_spec, out_spec), check_vma=False)
```

```python
import functools
import jax
import jax.numpy as jnp
from jax import lax
from jax.experimental import pallas as pl
from jax.experimental.pallas import tpu as pltpu
from jax.sharding import PartitionSpec as P

HIGHEST = lax.Precision.HIGHEST
MESH = pl.DeviceIdType.MESH
LEAF = 8
GROUP = 2
AHEAD = 2
BLK = 128
GRAM_TILES = (1024, 1024, 1024)
BASIS_TILES = (512, 1024, 2048)
VMEM_BYTES = 64000 * 1024


def dot_f32(lhs, rhs, lhs_dim, rhs_dim):
    return lax.dot_general(lhs, rhs, (((lhs_dim,), (rhs_dim,)), ((), ())), precision=HIGHEST, preferred_element_type=jnp.float32)


class RowSum:
    def __init__(self, members, sizes, part, out, pair_buf, acc, slots, sems):
        self.chips = members // 2
        me = lax.axis_index("rows")
        self.core, self.chip = lax.rem(me, 2), lax.div(me, 2)
        self.sizes = sizes
        self.starts = [sum(sizes[:g]) for g in range(len(sizes))]
        self.part, self.out, self.pair_buf, self.acc, self.slots = part, out, pair_buf, acc, slots
        self.swap_send, self.swap_recv, self.send, self.recv, self.back_send, self.back_recv, self.fwd_send, self.fwd_recv = sems

    def peer(self, d):
        return lax.rem(self.chip + d, self.chips)

    def pair_id(self):
        return {"rows": self.chip * 2 + 1 - self.core}

    def peer_id(self, d):
        return {"rows": self.peer(d) * 2 + self.core}

    def greet(self):
        barrier = pltpu.get_barrier_semaphore()
        pl.semaphore_signal(barrier, inc=1, device_id=self.pair_id(), device_id_type=MESH)
        for d in range(1, self.chips):
            pl.semaphore_signal(barrier, inc=1, device_id=self.peer_id(d), device_id_type=MESH)

    def await_all(self):
        pl.semaphore_wait(pltpu.get_barrier_semaphore(), self.chips)

    def half_rows(self, g, core):
        half = self.sizes[g] * BLK // 2
        return pl.ds(pl.multiple_of(self.starts[g] * BLK + core * half, 8), half)

    def chunk_of(self, g):
        return self.sizes[g] * BLK // (2 * self.chips)

    def own_rows(self, g, chip):
        half, chunk = self.sizes[g] * BLK // 2, self.chunk_of(g)
        return pl.ds(pl.multiple_of(self.starts[g] * BLK + self.core * half + chip * chunk, 8), chunk)

    def local_rows(self, g, chip):
        chunk = self.chunk_of(g)
        return pl.ds(pl.multiple_of(self.starts[g] * BLK // 2 + chip * chunk, 8), chunk)

    def local_half(self, g):
        return pl.ds(self.starts[g] * BLK // 2, self.sizes[g] * BLK // 2)

    def slot(self, g, d):
        chunk = self.chunk_of(g)
        base = self.starts[g] * BLK // (2 * self.chips)
        return self.slots.at[d - 1, pl.ds(base, chunk)]

    def swap(self, g):
        return pltpu.make_async_remote_copy(
            src_ref=self.part.at[self.half_rows(g, 1 - self.core)], dst_ref=self.pair_buf.at[self.local_half(g)],
            send_sem=self.swap_send.at[g], recv_sem=self.swap_recv.at[g], device_id=self.pair_id(), device_id_type=MESH)

    def scatter(self, g, d):
        return pltpu.make_async_remote_copy(
            src_ref=self.acc.at[self.local_rows(g, self.peer(d))], dst_ref=self.slot(g, d),
            send_sem=self.send.at[g, d - 1], recv_sem=self.recv.at[g, d - 1], device_id=self.peer_id(d), device_id_type=MESH)

    def gather(self, g, d):
        own = self.own_rows(g, self.chip)
        return pltpu.make_async_remote_copy(
            src_ref=self.out.at[own], dst_ref=self.out.at[own],
            send_sem=self.back_send.at[g, d - 1], recv_sem=self.back_recv.at[g, d - 1], device_id=self.peer_id(d), device_id_type=MESH)

    def forward(self, g, d):
        src = self.own_rows(g, self.peer(self.chips - d))
        return pltpu.make_async_remote_copy(
            src_ref=self.out.at[src], dst_ref=self.out.at[src],
            send_sem=self.fwd_send.at[g, d], recv_sem=self.fwd_recv.at[g, d], device_id=self.pair_id(), device_id_type=MESH)

    def start_swap(self, g):
        self.swap(g).start()

    def start_scatter(self, g):
        self.swap(g).wait()
        self.acc[self.local_half(g), :] = self.part[self.half_rows(g, self.core), :] + self.pair_buf[self.local_half(g), :]
        for d in range(1, self.chips):
            self.scatter(g, d).start()

    def start_gather(self, g):
        for d in range(1, self.chips):
            self.scatter(g, d).wait()
        total = self.acc[self.local_rows(g, self.chip), :]
        for d in range(1, self.chips):
            total = total + self.slot(g, d)[...]
        self.out[self.own_rows(g, self.chip), :] = total
        for d in range(1, self.chips):
            self.gather(g, d).start()
        self.forward(g, 0).start()

    def start_forward(self, g):
        for d in range(1, self.chips):
            self.gather(g, d).wait()
            self.forward(g, d).start()

    def drain(self, g):
        for d in range(self.chips):
            self.forward(g, d).wait()


def sum_scratch(members, sizes):
    chips = members // 2
    rows = sum(sizes) * BLK
    groups = len(sizes)
    sems = pltpu.SemaphoreType.DMA
    return [
        pltpu.VMEM((rows, BLK), jnp.float32), pltpu.VMEM((rows // 2, BLK), jnp.float32), pltpu.VMEM((rows // 2, BLK), jnp.float32),
        pltpu.VMEM((chips - 1, rows // (2 * chips), BLK), jnp.float32),
        sems((groups,)), sems((groups,)), sems((groups, chips - 1)), sems((groups, chips - 1)),
        sems((groups, chips - 1)), sems((groups, chips - 1)), sems((groups, chips)), sems((groups, chips)),
    ]


GRAM_GROUPS = (
    ((0, 2), (0, 3), (1, 2), (1, 3), (2, 2), (2, 3), (3, 3), (4, 2), (4, 3)),
    ((0, 0), (0, 1), (1, 1), (4, 0), (4, 1)),
    ((4, 4),),
)
BASIS_GROUPS = (
    ((0, 4), (1, 4), (2, 4), (3, 4), (4, 4)),
    ((0, 2), (0, 3), (1, 2), (1, 3), (2, 2), (2, 3), (3, 3)),
    ((0, 0), (0, 1), (1, 1)),
)


def proj_blocks(n):
    return -(-(n // 2) // BLK)


def block(idx):
    return slice(idx * BLK, (idx + 1) * BLK)


def pack_group(acc, part, start, pairs):
    for pos, (i, j) in enumerate(pairs):
        part[block(start + pos), :] = acc[block(i), block(j)] if i <= j else acc[block(i), block(j)].T


def tile_rows(t, size):
    return pl.ds(pl.multiple_of(t * size, size), size)


def tile_copy(src, dst, sem, t, size):
    rows = tile_rows(t, size)
    return pltpu.make_async_copy(src.at[rows], dst.at[rows], sem.at[t])


def gram_kernel(members, a_hbm, out, a_buf, acc, load_sem, part, pair_buf, acc_half, slots, *sems):
    first_size, second_size, third_size = GRAM_TILES
    tiles = a_buf.shape[0] // first_size
    sizes = [len(group) for group in GRAM_GROUPS]
    total = RowSum(members, sizes, part, out, pair_buf, acc_half, slots, sems)
    total.greet()
    for t in range(tiles):
        tile_copy(a_hbm, a_buf, load_sem, t, first_size).start()
    acc[...] = jnp.zeros_like(acc)

    def first(t, carry):
        tile_copy(a_hbm, a_buf, load_sem, t, first_size).wait()
        rows = tile_rows(t, first_size)
        acc[:, 2 * BLK:4 * BLK] += dot_f32(a_buf[rows, :], a_buf[rows, 2 * BLK:4 * BLK], 0, 0)
        return carry

    lax.fori_loop(0, tiles, first, 0)
    pack_group(acc, part, total.starts[0], GRAM_GROUPS[0])
    total.await_all()
    total.start_swap(0)

    def second(t, carry):
        @pl.when(t == 1)
        def _():
            total.start_scatter(0)

        rows = tile_rows(t, second_size)
        rhs = a_buf[rows, :2 * BLK]
        acc[:2 * BLK, :2 * BLK] += dot_f32(rhs, rhs, 0, 0)
        acc[4 * BLK:, :2 * BLK] += dot_f32(a_buf[rows, 4 * BLK:], rhs, 0, 0)
        return carry

    lax.fori_loop(0, a_buf.shape[0] // second_size, second, 0)
    pack_group(acc, part, total.starts[1], GRAM_GROUPS[1])
    total.start_swap(1)

    def third(t, carry):
        @pl.when(t == 0)
        def _():
            total.start_gather(0)

        @pl.when(t == 3)
        def _():
            total.start_scatter(1)

        last = a_buf[tile_rows(t, third_size), 4 * BLK:]
        acc[4 * BLK:, 4 * BLK:] += dot_f32(last, last, 0, 0)
        return carry

    lax.fori_loop(0, a_buf.shape[0] // third_size, third, 0)
    pack_group(acc, part, total.starts[2], GRAM_GROUPS[2])
    total.start_swap(2)
    total.start_scatter(2)
    total.start_gather(1)
    total.start_forward(0)
    total.start_gather(2)
    total.start_forward(1)
    total.start_forward(2)
    for g in range(3):
        total.drain(g)


def gram_sum(a_blk, members, collective_id):
    m, n = a_blk.shape
    sizes = [len(group) for group in GRAM_GROUPS]
    return pl.pallas_call(
        functools.partial(gram_kernel, members),
        out_shape=jax.ShapeDtypeStruct((sum(sizes) * BLK, BLK), jnp.float32),
        in_specs=[pl.BlockSpec(memory_space=pl.ANY)],
        out_specs=pl.BlockSpec(memory_space=pltpu.VMEM),
        scratch_shapes=[pltpu.VMEM((m, n), jnp.float32), pltpu.VMEM((n, n), jnp.float32), pltpu.SemaphoreType.DMA((m // GRAM_TILES[0],))] + sum_scratch(members, sizes),
        compiler_params=pltpu.CompilerParams(vmem_limit_bytes=VMEM_BYTES, collective_id=collective_id, has_side_effects=True),
        cost_estimate=pl.CostEstimate(flops=m * n * n * 6, bytes_accessed=4 * m * n, transcendentals=0),
        name="gram_one_sum",
    )(a_blk)


def basis_tile(a, inv, diag):
    left = dot_f32(a[:, :2 * BLK], inv[:2 * BLK, :2 * BLK], 1, 0)
    right = dot_f32(a[:, :4 * BLK], inv[:4 * BLK, 3 * BLK:], 1, 0)
    middle = dot_f32(a[:, :2 * BLK], inv[:2 * BLK, 2 * BLK:3 * BLK], 1, 0)
    ends = dot_f32(jnp.concatenate([a[:, 2 * BLK:3 * BLK], a[:, 4 * BLK:]], axis=1), diag[...], 1, 0)
    return left, middle + ends[:, :BLK], right[:, :BLK], right[:, BLK:] + ends[:, BLK:]


def basis_kernel(members, a_hbm, b_hbm, inv, out, a_buf, b_buf, diag, acc, acc_end, load_sem, b_sem, part, pair_buf, acc_half, slots, *sems):
    first_size, second_size, third_size = BASIS_TILES
    tiles = a_buf.shape[0] // first_size
    n, n_rhs = a_buf.shape[1], b_buf.shape[0]
    sizes = [len(group) for group in BASIS_GROUPS]
    n_end = sizes[0]
    sizes[0] += proj_blocks(n)
    total = RowSum(members, sizes, part, out, pair_buf, acc_half, slots, sems)
    total.greet()
    tile_copy(a_hbm, a_buf, load_sem, 0, first_size).start()
    b_copy = pltpu.make_async_copy(b_hbm, b_buf, b_sem)
    b_copy.start()
    for t in range(1, tiles):
        tile_copy(a_hbm, a_buf, load_sem, t, first_size).start()
    acc[...] = jnp.zeros_like(acc)
    acc_end[...] = jnp.zeros_like(acc_end)
    diag[...] = jnp.zeros_like(diag)
    diag[:BLK, :BLK] = inv[2 * BLK:3 * BLK, 2 * BLK:3 * BLK]
    diag[BLK:, BLK:] = inv[4 * BLK:, 4 * BLK:]
    b_copy.wait()

    def first(t, carry):
        tile_copy(a_hbm, a_buf, load_sem, t, first_size).wait()
        rows = tile_rows(t, first_size)
        left, third, fourth, fifth = basis_tile(a_buf[rows, :], inv, diag)
        a_buf[rows, :2 * BLK] = left
        a_buf[rows, 2 * BLK:3 * BLK] = third
        a_buf[rows, 3 * BLK:4 * BLK] = fourth
        a_buf[rows, 4 * BLK:] = fifth
        both = jnp.concatenate([fifth, b_buf[:, tile_rows(t, first_size)].T], axis=1)
        acc_end[...] += dot_f32(a_buf[rows, :], both, 0, 0)
        return carry

    lax.fori_loop(0, tiles, first, 0)
    for pos, (i, _) in enumerate(BASIS_GROUPS[0]):
        part[block(pos), :] = acc_end[block(i), :BLK]
    half = n // 2
    base = n_end * BLK
    part[base:base + half, :] = jnp.concatenate([acc_end[:half, BLK:], acc_end[half:, BLK:]], axis=1)
    if base + half < sizes[0] * BLK:
        part[base + half:sizes[0] * BLK, :] = jnp.zeros((sizes[0] * BLK - base - half, BLK), jnp.float32)
    total.await_all()
    total.start_swap(0)

    def second(t, carry):
        @pl.when(t == 1)
        def _():
            total.start_scatter(0)

        @pl.when(t == 6)
        def _():
            total.start_gather(0)

        rows = tile_rows(t, second_size)
        acc[:, 2 * BLK:] += dot_f32(a_buf[rows, :4 * BLK], a_buf[rows, 2 * BLK:4 * BLK], 0, 0)
        return carry

    lax.fori_loop(0, a_buf.shape[0] // second_size, second, 0)
    pack_group(acc, part, total.starts[1], BASIS_GROUPS[1])
    total.start_swap(1)

    def third_part(t, carry):
        @pl.when(t == 1)
        def _():
            total.start_scatter(1)

        rows = tile_rows(t, third_size)
        rhs = a_buf[rows, :2 * BLK]
        acc[:2 * BLK, :2 * BLK] += dot_f32(rhs, rhs, 0, 0)
        return carry

    lax.fori_loop(0, a_buf.shape[0] // third_size, third_part, 0)
    pack_group(acc, part, total.starts[2], BASIS_GROUPS[2])
    total.start_swap(2)
    total.start_scatter(2)
    total.start_forward(0)
    total.start_gather(1)
    total.start_gather(2)
    total.start_forward(1)
    total.start_forward(2)
    for g in range(3):
        total.drain(g)


def basis_sum(a_blk, b_blk, r_inv, members, collective_id):
    m, n = a_blk.shape
    n_rhs = b_blk.shape[1]
    sizes = [len(group) for group in BASIS_GROUPS]
    sizes[0] += proj_blocks(n)
    any_spec, vmem_spec = pl.BlockSpec(memory_space=pl.ANY), pl.BlockSpec(memory_space=pltpu.VMEM)
    return pl.pallas_call(
        functools.partial(basis_kernel, members),
        out_shape=jax.ShapeDtypeStruct((sum(sizes) * BLK, BLK), jnp.float32),
        in_specs=[any_spec, any_spec, vmem_spec],
        out_specs=vmem_spec,
        scratch_shapes=[
            pltpu.VMEM((m, n), jnp.float32), pltpu.VMEM((n_rhs, m), jnp.float32), pltpu.VMEM((2 * BLK, 2 * BLK), jnp.float32),
            pltpu.VMEM((4 * BLK, 4 * BLK), jnp.float32), pltpu.VMEM((n, BLK + n_rhs), jnp.float32),
            pltpu.SemaphoreType.DMA((m // BASIS_TILES[0],)), pltpu.SemaphoreType.DMA,
        ] + sum_scratch(members, sizes),
        compiler_params=pltpu.CompilerParams(vmem_limit_bytes=VMEM_BYTES, collective_id=collective_id, has_side_effects=True),
        cost_estimate=pl.CostEstimate(flops=m * n * n * 12, bytes_accessed=4 * m * (n + n_rhs), transcendentals=0),
        name="basis_gram_two_sum",
    )(a_blk, b_blk.T, r_inv)


def row_of(arr, idx):
    return jnp.broadcast_to(arr[idx:idx + 1, :], (LEAF, arr.shape[1]))


def factor_block(sym):
    n_leaf = BLK // LEAF
    row_id = lax.broadcasted_iota(jnp.int32, (BLK, BLK), 0)
    col_id = lax.broadcasted_iota(jnp.int32, (BLK, BLK), 1)
    eye = (row_id == col_id).astype(jnp.float32)
    sub_id = lax.broadcasted_iota(jnp.int32, (LEAF, BLK), 0)
    s_rows = [sym[LEAF * t:LEAF * (t + 1), :] for t in range(n_leaf)]
    i_rows = [eye[LEAF * t:LEAF * (t + 1), :] for t in range(n_leaf)]
    for t in range(0, n_leaf, GROUP):
        first = LEAF * t
        span = list(range(t, min(t + GROUP + AHEAD, n_leaf)))
        ecol = [[jnp.broadcast_to(s_rows[u][:, first + j:first + j + 1], (LEAF, BLK)) if u >= t + j // LEAF else None for u in span] for j in range(GROUP * LEAF)]
        done_s, done_i = list(s_rows[t:t + GROUP]), list(i_rows[t:t + GROUP])
        for i in range(GROUP * LEAF):
            v0, sub = i // LEAF, i % LEAF
            inv = lax.rsqrt(row_of(ecol[i][v0], sub))
            lcol = [None] * v0 + [e * inv for e in ecol[i][v0:]]
            bc_s = row_of(s_rows[t + v0], sub) * inv
            bc_i = row_of(i_rows[t + v0], sub) * inv
            done_s[v0] = jnp.where(sub_id == sub, bc_s, done_s[v0])
            done_i[v0] = jnp.where(sub_id == sub, bc_i, done_i[v0])
            for v in range(v0, len(span)):
                if v == v0 and sub == LEAF - 1:
                    continue
                u = span[v]
                s_rows[u] = s_rows[u] - lcol[v] * bc_s
                i_rows[u] = i_rows[u] - lcol[v] * bc_i
            for j in range(i + 1, GROUP * LEAF):
                piv = row_of(lcol[j // LEAF], j % LEAF)
                for v in range(j // LEAF, len(span)):
                    ecol[j][v] = ecol[j][v] - lcol[v] * piv
        s_rows[t:t + GROUP], i_rows[t:t + GROUP] = done_s, done_i
        rest = t + GROUP + AHEAD
        if rest < n_leaf:
            w_s = jnp.concatenate(done_s, axis=0)
            upd = dot_f32(w_s, jnp.concatenate([w_s, jnp.concatenate(done_i, axis=0)], axis=1), 0, 0)
            for u in range(rest, n_leaf):
                s_rows[u] = s_rows[u] - upd[LEAF * u:LEAF * (u + 1), :BLK]
                i_rows[u] = i_rows[u] - upd[LEAF * u:LEAF * (u + 1), BLK:]
    r_blk = jnp.where(row_id <= col_id, jnp.concatenate(s_rows, axis=0), 0.0)
    linv = jnp.where(row_id >= col_id, jnp.concatenate(i_rows, axis=0), 0.0)
    return r_blk, linv


def factor_all(work, r_out, n):
    n_blk = n // BLK

    def step(k, carry):
        base = pl.multiple_of(k * BLK, BLK)
        r_blk, linv = factor_block(work[pl.ds(base, BLK), pl.ds(base, BLK)])
        for kk in range(n_blk):
            @pl.when(k == kk)
            def _():
                lo, hi = BLK * kk, BLK * (kk + 1)
                if lo:
                    work[lo:hi, :lo] = dot_f32(linv, work[lo:hi, :lo], 1, 0)
                    r_out[lo:hi, :lo] = jnp.zeros((BLK, lo), jnp.float32)
                work[lo:hi, lo:hi] = linv
                r_out[lo:hi, lo:hi] = r_blk
                if hi < n:
                    r_row = dot_f32(linv, work[lo:hi, hi:], 1, 0)
                    r_out[lo:hi, hi:] = r_row
                    work[lo:hi, hi:] = jnp.zeros((BLK, n - hi), jnp.float32)
                    for ii in range(kk + 1, n_blk):
                        a, b = BLK * ii, BLK * (ii + 1)
                        fac = r_row[:, a - hi:b - hi]
                        work[a:b, a:] = work[a:b, a:] - dot_f32(fac, r_row[:, a - hi:], 0, 0)
                        if lo:
                            work[a:b, :lo] = work[a:b, :lo] - dot_f32(fac, work[lo:hi, :lo], 0, 0)
                        work[a:b, lo:hi] = -dot_f32(fac, linv, 0, 0)
        return carry

    lax.fori_loop(0, n_blk, step, 0)


def unpack_upper(packed, work, groups, skip):
    start = 0
    for group in groups:
        for pos, (i, j) in enumerate(group):
            lo, hi = min(i, j), max(i, j)
            work[block(lo), block(hi)] = packed[block(start + pos), :]
        start += len(group) + (skip if group is groups[0] else 0)


def factor_kernel(packed, r_out, inv_out, work):
    n = work.shape[0]
    unpack_upper(packed, work, GRAM_GROUPS, 0)
    factor_all(work, r_out, n)
    for c in range(0, n, BLK):
        inv_out[:, c:c + BLK] = work[c:c + BLK, :].T


def factor_one(packed, n):
    return pl.pallas_call(
        factor_kernel,
        out_shape=[jax.ShapeDtypeStruct((n, n), jnp.float32)] * 2,
        in_specs=[pl.BlockSpec(memory_space=pltpu.VMEM)],
        out_specs=[pl.BlockSpec(memory_space=pltpu.VMEM)] * 2,
        scratch_shapes=[pltpu.VMEM((n, n), jnp.float32)],
        name="factor_one",
    )(packed)


def finish_kernel(packed, r_one, inv_one, x_out, r_out, work, r_two):
    n_rhs, n = x_out.shape
    unpack_upper(packed, work, BASIS_GROUPS, proj_blocks(n))
    factor_all(work, r_two, n)
    base = len(BASIS_GROUPS[0]) * BLK
    half = n // 2
    flat = packed[base:base + half, :]
    proj = jnp.concatenate([flat[:, :n_rhs].T, flat[:, n_rhs:].T], axis=1)
    proj_two = dot_f32(proj, work[...], 1, 1)
    back = dot_f32(proj_two, work[...], 1, 0)
    x_out[...] = dot_f32(back, inv_one[...], 1, 1)
    for lo in range(0, n, BLK):
        hi = lo + BLK
        if lo:
            r_out[lo:hi, :lo] = jnp.zeros((BLK, lo), jnp.float32)
        r_out[lo:hi, lo:] = dot_f32(r_two[lo:hi, lo:], r_one[lo:, lo:], 1, 0)


def finish(packed, r_one, inv_one, n_rhs):
    n = r_one.shape[0]
    return pl.pallas_call(
        finish_kernel,
        out_shape=[jax.ShapeDtypeStruct((n_rhs, n), jnp.float32), jax.ShapeDtypeStruct((n, n), jnp.float32)],
        in_specs=[pl.BlockSpec(memory_space=pltpu.VMEM)] * 3,
        out_specs=[pl.BlockSpec(memory_space=pltpu.VMEM)] * 2,
        scratch_shapes=[pltpu.VMEM((n, n), jnp.float32)] * 2,
        name="finish",
    )(packed, r_one, inv_one)


def solution(mesh):
    members = mesh.shape["rows"]

    def group_solve(a_blk, b_blk):
        n, n_rhs = a_blk.shape[1], b_blk.shape[1]
        gram_one = gram_sum(a_blk, members, 1)
        r_one, inv_one = factor_one(gram_one, n)
        gram_two = basis_sum(a_blk, b_blk, inv_one, members, 2)
        x_flat, r_factor = finish(gram_two, r_one, inv_one, n_rhs)
        return x_flat.T, r_factor

    row_spec = P(("batch", "rows"), None)
    out_spec = P("batch", None)
    return jax.shard_map(group_solve, mesh=mesh, in_specs=(row_spec, row_spec), out_specs=(out_spec, out_spec), check_vma=False)
```
